32 devices in a mesh: dp: 8 (over z, y), mp: 4 (over x, core).
Axes of the slice: x: 2, y: 2, z: 4, core: 2. Of those that a mesh axis runs over, the one named last changes fastest.
Arguments:
- series: bfloat16 [8192, 1280], P('dp'), may hold values from -6 to 6
- inner_weight: bfloat16 [1280, 1280], P('mp'), may hold values from -0.15625 to 0.15625
- inner_bias: float32 [1280], P('mp'), may hold values from -3 to 3
- outer_weight: bfloat16 [1280, 1280], P('mp'), may hold values from -0.15625 to 0.15625
- skip_weight: bfloat16 [1280, 1280], P('mp'), may hold values from -0.15625 to 0.15625
- outer_bias: float32 [1280], replicated, may hold values from -3 to 3
- targets: float32 [8192, 128], P('dp'), may hold values from -9 to 9
- levels: int32 [10], replicated, may hold values from 0 to 8
- counts: int32 [512], P('dp'), may hold values from 1 to 16
Outputs:
- input_grad: float32 [8192, 1280], P('dp', 'mp')
- inner_grad: float32 [1280, 1280], P(('mp', 'dp'))
- outer_grad: float32 [1280, 1280], P(('mp', 'dp'))
- skip_grad: float32 [1280, 1280], P(('mp', 'dp'))
- inbias_grad: float32 [1280], P(('mp', 'dp'))
- outbias_grad: float32 [1280], P('dp')
The draws below stay inside these ranges and needn't reach their ends.
All inputs are finite; a program needn't handle non-finite values.
Results may differ from the reference program's by a relative error of at most 0.0039.
Values may be sent and summed in bfloat16 or wider, within the bound.
No kernel may reach another device: no remote copies, remote signals or barrier semaphores. Data moves between devices by JAX's collectives and lax.ppermute only.
A program may use at most 64 MiB of HBM per device.

```python
import jax
import jax.numpy as jnp
from jax import lax

D = 1280
H = 1280
P_SIZE = 128
Q = 10
LEVELS = 9
PATCHES = 16
OUT = 1280
WINDOWS = 512
ROWS = 8192


def place_ends(drawn, key, low, high):
    place = [jax.random.randint(jax.random.fold_in(key, axis), (), 0, length) for axis, length in enumerate(drawn.shape)]
    widest = drawn.shape.index(max(drawn.shape))
    beside = place[:widest] + [(place[widest] + 1) % drawn.shape[widest]] + place[widest + 1:]
    return drawn.at[tuple(place)].set(low).at[tuple(beside)].set(high)


def steps_of(stream_key, shape, shards, least, high):
    def one(position, shards_of):
        steps = jax.random.uniform(jax.random.fold_in(jax.random.fold_in(stream_key, 6), position), (shards_of,), jnp.float32, least / len(shards), high / len(shards))
        return jnp.repeat(jnp.exp(steps), shape[position] // shards_of).reshape((-1,) + (1,) * (len(shape) - position - 1))

    factor_of = one(*shards[0])
    for cut in shards[1:]:
        factor_of = factor_of * one(*cut)
    return factor_of


def normal_values(key, extent, width, limit, split=(), kind=jnp.bfloat16):
    drawn = width * jax.random.normal(key, extent, jnp.float32)
    if split:
        drawn = drawn * steps_of(key, extent, split, -0.22, 0.18)
    return jnp.clip(drawn, -limit, limit).astype(kind)


def setup_inputs(seed: int = 0) -> dict:
    key_list = jax.random.split(jax.random.key(seed), 10)
    series = normal_values(key_list[0], (ROWS, D), 1.0, 6.0, ((0, 8),))
    inner_weight = normal_values(key_list[1], (H, D), D ** -0.5, 0.15625, ((0, 4),))
    inner_bias = normal_values(key_list[2], (H,), 1.0, 3.0, ((0, 4),), jnp.float32)
    outer_weight = normal_values(key_list[3], (H, OUT), H ** -0.5, 0.15625, ((0, 4),))
    skip_weight = normal_values(key_list[4], (D, OUT), D ** -0.5, 0.15625, ((0, 4),))
    outer_bias = normal_values(key_list[5], (OUT,), 0.7, 3.0, (), jnp.float32)
    targets = normal_values(key_list[6], (ROWS, P_SIZE), 1.5, 9.0, ((0, 8),), jnp.float32)
    levels = place_ends(jax.random.randint(key_list[7], (Q,), 0, LEVELS), jax.random.fold_in(key_list[7], 1), 0, LEVELS - 1).astype(jnp.int32)
    counts = place_ends(jax.random.randint(key_list[8], (WINDOWS,), 1, PATCHES + 1), jax.random.fold_in(key_list[8], 1), 1, PATCHES).astype(jnp.int32)
    return {"series": series, "inner_weight": inner_weight, "inner_bias": inner_bias, "outer_weight": outer_weight, "skip_weight": skip_weight, "outer_bias": outer_bias, "targets": targets, "levels": levels, "counts": counts}


huber_width = 0.5


def output_slope(predicted, target_rows, count_rows, levels):
    row_count = predicted.shape[0]
    window_count = count_rows.shape[0]
    patch_count = row_count // window_count
    horizon = target_rows.shape[1]
    quantiles = levels.shape[0]
    fraction = (levels.astype(jnp.float32) + 1.0) / (LEVELS + 1)
    level_cols = jnp.broadcast_to(fraction[None, :], (horizon, quantiles)).reshape(horizon * quantiles)
    spread = jnp.broadcast_to(target_rows[:, :, None], (row_count, horizon, quantiles)).reshape(row_count, horizon * quantiles)
    residue = spread - predicted
    slopes = jnp.where(residue >= 0, level_cols, 1.0 - level_cols) * jnp.clip(residue / huber_width, -1.0, 1.0)
    positions = lax.broadcasted_iota(jnp.int32, (window_count, patch_count), 1)
    validity = (positions < count_rows[:, None]).astype(jnp.float32)
    weights = (validity / count_rows[:, None].astype(jnp.float32)).reshape(row_count, 1)
    return (-slopes * weights).astype(jnp.bfloat16)


def reference(series, inner_weight, inner_bias, outer_weight, skip_weight, outer_bias, targets, levels, counts):
    preact = jnp.dot(series, inner_weight.T, preferred_element_type=jnp.float32) + inner_bias
    sigmoids = jax.nn.sigmoid(preact)
    hidden = (preact * sigmoids).astype(jnp.bfloat16)
    predicted = jnp.dot(hidden, outer_weight, preferred_element_type=jnp.float32) + jnp.dot(series, skip_weight, preferred_element_type=jnp.float32) + outer_bias
    out_grad = output_slope(predicted, targets, counts, levels)
    backflow = jnp.dot(out_grad, outer_weight.T, preferred_element_type=jnp.float32)
    hidden_grad = (backflow * sigmoids * (1.0 + preact * (1.0 - sigmoids))).astype(jnp.bfloat16)
    input_grad = jnp.dot(hidden_grad, inner_weight, preferred_element_type=jnp.float32) + jnp.dot(out_grad, skip_weight.T, preferred_element_type=jnp.float32)
    rescale = 1.0 / WINDOWS
    inner_grad = jnp.dot(hidden_grad.T, series, preferred_element_type=jnp.float32) * rescale
    outer_grad = jnp.dot(hidden.T, out_grad, preferred_element_type=jnp.float32) * rescale
    skip_grad = jnp.dot(series.T, out_grad, preferred_element_type=jnp.float32) * rescale
    inbias_grad = jnp.sum(hidden_grad.astype(jnp.float32), axis=0) * rescale
    outbias_grad = jnp.sum(out_grad.astype(jnp.float32), axis=0) * rescale
    return (input_grad, inner_grad, outer_grad, skip_grad, inbias_grad, outbias_grad)
```

```python
import jax
import jax.numpy as jnp
from jax import lax
from jax.sharding import PartitionSpec as P

LEVELS = 9


huber_width = 0.5


def swap(value, axis, distance):
    size = lax.axis_size(axis)
    return lax.ppermute(value, axis, [(i, i ^ distance) for i in range(size)])


def output_slope(predicted, spread, weights, level_cols):
    residue = spread - predicted
    slopes = jnp.where(residue >= 0, level_cols, 1.0 - level_cols) * jnp.clip(
        residue / huber_width, -1.0, 1.0
    )
    return (-slopes * weights).astype(jnp.bfloat16)


def halve(blocks, axis, wire):
    index = lax.axis_index(axis)
    distance = 1
    while distance < lax.axis_size(axis):
        bit = (index // distance) % 2
        pairs = blocks.reshape((blocks.shape[0] // 2, 2) + blocks.shape[1:])
        sent = lax.dynamic_index_in_dim(pairs, 1 - bit, 1, keepdims=False).astype(wire)
        kept = lax.dynamic_index_in_dim(pairs, bit, 1, keepdims=False)
        blocks = kept + swap(sent, axis, distance).astype(jnp.float32)
        distance *= 2
    return blocks[0]


def on_device(
    series, inner_weight, inner_bias, outer_weight, skip_weight, outer_bias, targets, levels, counts
):
    f32, bf16 = jnp.float32, jnp.bfloat16
    row_count = series.shape[0]
    window_count = counts.shape[0]
    patch_count = row_count // window_count
    horizon = targets.shape[1]
    quantiles = levels.shape[0]
    out_width = horizon * quantiles
    slice_width = skip_weight.shape[0]
    model_index = lax.axis_index("mp")
    data_size = lax.axis_size("dp")
    core = model_index % 2
    half = row_count // 2
    on_last = (((1,), (1,)), ((), ()))
    over_rows = (((0,), (0,)), ((), ()))
    own_series = lax.dynamic_slice_in_dim(series, model_index * slice_width, slice_width, 1)

    fraction = (levels.astype(f32) + 1.0) / (LEVELS + 1)
    level_cols = jnp.broadcast_to(fraction[None, :], (horizon, quantiles)).reshape(out_width)
    own_targets = lax.dynamic_slice_in_dim(targets, core * half, half, 0)
    spread = jnp.broadcast_to(own_targets[:, :, None], (half, horizon, quantiles)).reshape(
        half, out_width
    )
    positions = lax.broadcasted_iota(jnp.int32, (window_count, patch_count), 1)
    validity = (positions < counts[:, None]).astype(f32)
    weights = (validity / counts[:, None].astype(f32)).reshape(row_count, 1)
    own_weights = lax.dynamic_slice_in_dim(weights, core * half, half, 0)

    preact = lax.dot_general(series, inner_weight, on_last, preferred_element_type=f32) + inner_bias
    sigmoids = jax.nn.sigmoid(preact)
    hidden = (preact * sigmoids).astype(bf16)
    partial_out = jnp.dot(hidden, outer_weight, preferred_element_type=f32) + jnp.dot(
        own_series, skip_weight, preferred_element_type=f32
    )
    sent = lax.dynamic_slice_in_dim(partial_out, (1 - core) * half, half, 0).astype(bf16)
    kept = lax.dynamic_slice_in_dim(partial_out, core * half, half, 0)
    chip_part = (kept + swap(sent, "mp", 1).astype(f32)).astype(bf16)

    chunks = 2
    width = out_width // chunks
    backflow = None
    skip_part = None
    outer_blocks = []
    outbias_parts = []
    for chunk in range(chunks):
        cols = slice(chunk * width, (chunk + 1) * width)
        own = chip_part[:, cols]
        predicted = own.astype(f32) + swap(own, "mp", 2).astype(f32) + outer_bias[cols]
        mine = output_slope(predicted, spread[:, cols], own_weights, level_cols[cols])
        theirs = swap(mine, "mp", 1)
        out_grad = jnp.where(
            core == 0,
            jnp.concatenate([mine, theirs], 0),
            jnp.concatenate([theirs, mine], 0),
        )
        outer_part = lax.dot_general(hidden, out_grad, over_rows, preferred_element_type=f32)
        skip_grad_part = lax.dot_general(
            own_series, out_grad, over_rows, preferred_element_type=f32
        )
        outer_blocks.append(
            halve(
                jnp.stack(
                    [
                        outer_part.reshape(data_size, -1, width),
                        skip_grad_part.reshape(data_size, -1, width),
                    ],
                    1,
                ),
                "dp",
                bf16,
            )
        )
        outbias_parts.append(jnp.sum(out_grad, axis=0, dtype=f32))
        flow = lax.dot_general(
            out_grad, outer_weight[:, cols], on_last, preferred_element_type=f32
        )
        backflow = flow if backflow is None else backflow + flow
        through = lax.dot_general(
            out_grad, skip_weight[:, cols], on_last, preferred_element_type=f32
        )
        skip_part = through if skip_part is None else skip_part + through
    hidden_grad = (backflow * sigmoids * (1.0 + preact * (1.0 - sigmoids))).astype(bf16)
    inner_part = lax.dot_general(hidden_grad, series, over_rows, preferred_element_type=f32)
    inner_block = halve(inner_part.reshape(data_size, -1, inner_part.shape[1]), "dp", bf16)
    inbias_part = jnp.sum(hidden_grad, axis=0, dtype=f32)
    outbias_part = jnp.concatenate(outbias_parts)
    bias_block = halve(
        jnp.concatenate(
            [inbias_part.reshape(data_size, -1), outbias_part.reshape(data_size, -1)], 1
        ),
        "dp",
        f32,
    )
    spread_part = jnp.dot(hidden_grad, inner_weight, preferred_element_type=f32)
    input_blocks = jnp.moveaxis(
        spread_part.reshape(row_count, lax.axis_size("mp"), slice_width), 1, 0
    )
    input_total = halve(input_blocks, "mp", bf16) + skip_part

    rescale = 1.0 / (window_count * data_size)
    inbias_width = inbias_part.shape[0] // data_size
    outer_total = jnp.concatenate([b[0] for b in outer_blocks], 1)
    skip_total = jnp.concatenate([b[1] for b in outer_blocks], 1)
    return (
        input_total,
        inner_block * rescale,
        outer_total * rescale,
        skip_total * rescale,
        bias_block[:inbias_width] * rescale,
        bias_block[inbias_width:] * rescale,
    )


def solution(mesh):
    in_specs = (
        P("dp", None),
        P("mp", None),
        P("mp"),
        P("mp", None),
        P("mp", None),
        P(),
        P("dp", None),
        P(),
        P("dp"),
    )
    out_specs = (
        P("dp", "mp"),
        P(("mp", "dp"), None),
        P(("mp", "dp"), None),
        P(("mp", "dp"), None),
        P(("mp", "dp")),
        P("dp"),
    )
    return jax.shard_map(
        on_device, mesh=mesh, in_specs=in_specs, out_specs=out_specs, check_vma=False
    )
```

```python
import functools

import jax
import jax.numpy as jnp
from jax import lax
from jax.experimental import pallas as pl
from jax.experimental.pallas import tpu as pltpu
from jax.sharding import PartitionSpec as P

LEVELS = 9


huber_width = 0.5


F32, BF16 = jnp.float32, jnp.bfloat16
LANES = 128
ROW_BLOCK = 256
ON_LAST = (((1,), (1,)), ((), ()))
IN_VMEM = pl.BlockSpec(memory_space=pltpu.VMEM)


def dot(a, b):
    return jnp.dot(a, b, preferred_element_type=F32)


def dot_last(a, b):
    return lax.dot_general(a, b, ON_LAST, preferred_element_type=F32)


def round_up(value, step):
    return -(-value // step) * step


def call(body, shapes, *args, flops, scratch=(), vmem=24 << 20):
    moved = sum(a.size * a.dtype.itemsize for a in args)
    moved += sum(s.size * s.dtype.itemsize for s in shapes)
    return pl.pallas_call(
        body,
        out_shape=tuple(shapes),
        in_specs=[IN_VMEM] * len(args),
        out_specs=tuple(IN_VMEM for _ in shapes),
        scratch_shapes=list(scratch),
        cost_estimate=pl.CostEstimate(
            flops=int(flops), bytes_accessed=int(moved), transcendentals=0
        ),
        compiler_params=pltpu.CompilerParams(vmem_limit_bytes=vmem),
    )(*args)


def shape(dims, dtype):
    return jax.ShapeDtypeStruct(dims, dtype)


def swap(value, axis, distance):
    size = lax.axis_size(axis)
    return lax.ppermute(value, axis, [(i, i ^ distance) for i in range(size)])


class Window:
    def __init__(self, width, parts):
        gap = max((part * width) % LANES for part in range(parts))
        self.at = round_up(width, LANES)
        self.width = round_up(width + gap, LANES)
        self.total = self.at + self.width

    def place(self, part, width):
        first = part * width
        start = first // LANES * LANES
        return pl.multiple_of(start, LANES), first - start


def forward(window, series, wi, bias, wo, ws, joined, slope_in, joined_w, *parts):
    sent, kept = parts[: len(parts) // 2], parts[len(parts) // 2 :]
    units, width = wi.shape[0], ws.shape[0]
    part = lax.axis_index("mp")
    core = part % 2
    half = series.shape[0] // 2
    block = min(ROW_BLOCK, half)
    start, gap = window.place(part, width)
    joined_w[...] = jnp.zeros_like(joined_w)
    joined_w[0:units, :] = wo[...]
    joined_w[pl.ds(pl.multiple_of(window.at + gap, 16), width), :] = ws[...]

    def rows_to(base, targets):
        def step(i, _):
            at = pl.multiple_of(i * block, block)
            rows = pl.ds(pl.multiple_of(base + at, block), block)
            preact = dot_last(series[rows, :], wi[...]) + bias[...]
            sigmoids = 1.0 / (1.0 + jnp.exp(-preact))
            slope_in[rows, :] = sigmoids * (1.0 + preact * (1.0 - sigmoids))
            if units < window.at:
                joined[rows, units : window.at] = jnp.zeros(
                    (block, window.at - units), BF16
                )
            joined[rows, 0:units] = (preact * sigmoids).astype(BF16)
            joined[rows, window.at : window.total] = series[rows, pl.ds(start, window.width)]
            mixed = joined[rows, :]
            first = 0
            for target in targets:
                cols = slice(first, first + target.shape[1])
                target[pl.ds(at, block), :] = dot(mixed, joined_w[:, cols]).astype(target.dtype)
                first += target.shape[1]
            return 0

        lax.fori_loop(0, half // block, step, 0)

    rows_to((1 - core) * half, sent)
    rows_to(core * half, kept)


def slope(first_col, patch_count, own, other, bias, targets, level, counts, grad):
    half, width = own.shape
    horizon = targets.shape[1]
    quantiles = level.shape[1]
    core = lax.axis_index("mp") % 2
    block = min(ROW_BLOCK, half)
    columns = lax.broadcasted_iota(jnp.int32, (horizon, width), 1) + first_col
    lowest = lax.broadcasted_iota(jnp.int32, (horizon, width), 0) * quantiles
    chosen = jnp.where((columns >= lowest) & (columns < lowest + quantiles), 1.0, 0.0)
    chosen = chosen.astype(BF16)
    channel = lax.broadcasted_iota(jnp.int32, (1, width), 1) + first_col
    channel = lax.rem(channel, quantiles)
    picked = jnp.zeros((1, width), jnp.int32)
    for c in range(quantiles):
        picked = jnp.where(channel == c, level[0:1, c : c + 1], picked)
    above = (picked.astype(F32) + 1.0) / (LEVELS + 1)
    below = 1.0 - above
    count = counts[...]
    inverse = 1.0 / count.astype(F32)

    def step(i, _):
        at = pl.multiple_of(i * block, block)
        rows = pl.ds(at, block)
        base = pl.multiple_of(core * half + at, block)
        target = targets[pl.ds(base, block), :]
        high = target.astype(BF16)
        rest = target - high.astype(F32)
        middle = rest.astype(BF16)
        low = (rest - middle.astype(F32)).astype(BF16)
        spread = dot(high, chosen) + dot(middle, chosen) + dot(low, chosen)
        predicted = own[rows, :].astype(F32) + other[rows, :].astype(F32) + bias[...]
        residue = spread - predicted
        slopes = jnp.where(residue >= 0, above, below) * jnp.clip(
            residue / huber_width, -1.0, 1.0
        )
        row = lax.broadcasted_iota(jnp.int32, (block, count.shape[1]), 0) + base
        opens = lax.broadcasted_iota(jnp.int32, (block, count.shape[1]), 1) * patch_count
        inside = (row >= opens) & (row < opens + count)
        weights = jnp.sum(jnp.where(inside, inverse, 0.0), axis=1, keepdims=True)
        grad[rows, :] = (-slopes * weights).astype(BF16)
        return 0

    lax.fori_loop(0, half // block, step, 0)


def split(total, at, sent, kept, bit):
    for pair in range(kept.shape[1]):
        depth = kept.shape[2]
        for target, which in ((sent, 1 - bit), (kept, bit)):
            rows = pl.ds(pl.multiple_of((2 * pair + which) * depth, 8), depth)
            target[at, pair] = total[rows, :].astype(target.dtype)


def outer_sums(window, units, joined_t, mine, theirs, sent, kept, total):
    half = mine.shape[0]
    part = lax.axis_index("mp")
    core = part % 2
    bit = lax.axis_index("dp") % 2
    _, gap = window.place(part, units)
    own = pl.ds(pl.multiple_of(core * half, half), half)
    far = pl.ds(pl.multiple_of((1 - core) * half, half), half)
    for at, first in ((0, 0), (1, pl.multiple_of(window.at + gap, 16))):
        rows = pl.ds(first, units)
        total[...] = dot(joined_t[rows, own], mine[...]) + dot(joined_t[rows, far], theirs[...])
        split(total, at, sent, kept, bit)


def back(weight, mine, theirs, flow):
    half = mine.shape[0]
    core = lax.axis_index("mp") % 2
    for grads, which in ((mine, core), (theirs, 1 - core)):
        cols = pl.ds(pl.multiple_of(which * half, half), half)
        flow[:, cols] = dot_last(weight[...], grads[...])


def hidden_back(weight, mine, theirs, flow, slope_t, series, grad_t, sums, sent, kept, total):
    half = mine.shape[0]
    core = lax.axis_index("mp") % 2
    bit = lax.axis_index("dp") % 2
    for grads, which in ((mine, core), (theirs, 1 - core)):
        cols = pl.ds(pl.multiple_of(which * half, half), half)
        flown = flow[:, cols] + dot_last(weight[...], grads[...])
        grad_t[:, cols] = (flown * slope_t[:, cols]).astype(BF16)
    total[...] = dot(grad_t[...], series[...])
    split(total, 0, sent, kept, bit)
    summed = jnp.sum(grad_t[...].astype(F32), axis=1, keepdims=True)
    sums[...] = jnp.broadcast_to(summed, sums.shape)


def input_parts(weight_t, grad_t, sent, kept):
    core = lax.axis_index("mp") % 2
    width = kept.shape[2]
    for pair in range(kept.shape[1]):
        for target, which in ((sent, 1 - core), (kept, core)):
            rows = pl.ds(pl.multiple_of((2 * pair + which) * width, 16), width)
            target[0, pair] = dot(weight_t[rows, :], grad_t[...]).astype(target.dtype)


def skip_back(weight, width, *refs):
    grads, out = refs[:-1], refs[-1]
    half = grads[0].shape[0]
    core = lax.axis_index("mp") % 2
    for side, which in ((0, core), (1, 1 - core)):
        rows = pl.ds(pl.multiple_of(which * half, half), half)
        total = None
        for chunk in range(len(grads) // 2):
            cols = slice(chunk * width, (chunk + 1) * width)
            term = dot_last(grads[2 * chunk + side][...], weight[:, cols])
            total = term if total is None else total + term
        out[rows, :] = total


def halve_step(axis, distance, blocks, arrived, sent, kept):
    bit = (lax.axis_index(axis) // distance) % 2
    for at in range(kept.shape[0]):
        for pair in range(kept.shape[1]):
            for target, which in ((sent, 1 - bit), (kept, bit)):
                index = 2 * pair + which
                target[at, pair] = (
                    blocks[at, index] + arrived[at, index].astype(F32)
                ).astype(target.dtype)


def halve(sent, kept, axis, distance=1):
    while True:
        arrived = swap(sent, axis, distance)
        distance *= 2
        if distance >= lax.axis_size(axis):
            return kept, arrived
        dims = (kept.shape[0], kept.shape[1] // 2) + kept.shape[2:]
        sent, kept = call(
            functools.partial(halve_step, axis, distance),
            (shape(dims, BF16), shape(dims, F32)),
            kept,
            arrived,
            flops=kept.size,
        )


def last_sums(rescale, *refs):
    count = (len(refs) - 3) // 2
    kept, arrived, outs = refs[:count], refs[count : 2 * count], refs[2 * count :]
    outs[0][...] = (kept[0][0, 0] + arrived[0][0, 0].astype(F32)) * rescale
    for at in range(2):
        first = 0
        for k, a in zip(kept[1:], arrived[1:]):
            cols = slice(first, first + k.shape[3])
            outs[1 + at][:, cols] = (k[at, 0] + a[at, 0].astype(F32)) * rescale
            first += k.shape[3]


def halve_small(blocks, axis):
    index = lax.axis_index(axis)
    distance = 1
    while distance < lax.axis_size(axis):
        bit = (index // distance) % 2
        pairs = blocks.reshape((blocks.shape[0] // 2, 2) + blocks.shape[1:])
        sent = lax.dynamic_index_in_dim(pairs, 1 - bit, 1, keepdims=False)
        kept = lax.dynamic_index_in_dim(pairs, bit, 1, keepdims=False)
        blocks = kept + swap(sent, axis, distance)
        distance *= 2
    return blocks[0]


def on_device(
    series, inner_weight, inner_bias, outer_weight, skip_weight, outer_bias, targets, levels, counts
):
    row_count, depth = series.shape
    window_count = counts.shape[0]
    patch_count = row_count // window_count
    out_width = outer_weight.shape[1]
    units = inner_weight.shape[0]
    model_size = lax.axis_size("mp")
    data_size = lax.axis_size("dp")
    half = row_count // 2
    window = Window(units, model_size)
    chunks = 2
    width = out_width // chunks
    pairs = data_size // 2
    share = units // data_size

    parts = [shape((half, width), F32)] * (2 * chunks)
    joined, slope_in, joined_w, *parts = call(
        functools.partial(forward, window),
        [
            shape((row_count, window.total), BF16),
            shape((row_count, units), F32),
            shape((window.total, out_width), BF16),
            *parts,
        ],
        series,
        inner_weight,
        inner_bias.reshape(1, units),
        outer_weight,
        skip_weight,
        flops=2 * row_count * depth * units + 2 * row_count * window.total * out_width,
        vmem=40 << 20,
    )
    own = [
        (kept + swap(sent, "mp", 1)).astype(BF16)
        for sent, kept in zip(parts[:chunks], parts[chunks:])
    ]
    other = [swap(value, "mp", 2) for value in own]
    joined_t = joined.T
    slope_t = slope_in.T
    inner_t = inner_weight.T

    grads = []
    halved = []
    flow = None
    for chunk in range(chunks):
        cols = slice(chunk * width, (chunk + 1) * width)
        (mine,) = call(
            functools.partial(slope, chunk * width, patch_count),
            [shape((half, width), BF16)],
            own[chunk],
            other[chunk],
            outer_bias[cols].reshape(1, width),
            targets,
            levels.reshape(1, -1),
            counts.reshape(1, -1),
            flops=6 * half * targets.shape[1] * width,
        )
        theirs = swap(mine, "mp", 1)
        grads += [mine, theirs]
        dims = (2, pairs, share, width)
        sent, kept = call(
            functools.partial(outer_sums, window, units),
            [shape(dims, BF16), shape(dims, F32)],
            joined_t,
            mine,
            theirs,
            flops=4 * row_count * units * width,
            scratch=[pltpu.VMEM((units, width), F32)],
        )
        halved.append(halve(sent, kept, "dp"))
        if chunk < chunks - 1:
            (flown,) = call(
                back,
                [shape((units, row_count), F32)],
                outer_weight[:, cols],
                mine,
                theirs,
                flops=2 * row_count * units * width,
            )
            flow = flown if flow is None else flow + flown
        else:
            dims = (1, pairs, share, depth)
            grad_t, inbias_part, sent, kept = call(
                hidden_back,
                [
                    shape((units, row_count), BF16),
                    shape((units, LANES), F32),
                    shape(dims, BF16),
                    shape(dims, F32),
                ],
                outer_weight[:, cols],
                mine,
                theirs,
                flow,
                slope_t,
                series,
                flops=4 * row_count * units * width,
                scratch=[pltpu.VMEM((units, depth), F32)],
            )
            halved.insert(0, halve(sent, kept, "dp"))
    dims = (1, model_size // 2, units, row_count)
    sent, kept = call(
        input_parts,
        [shape(dims, BF16), shape(dims, F32)],
        inner_t,
        grad_t,
        flops=2 * row_count * units * depth,
    )
    kept_t, arrived_t = halve(sent, kept, "mp")
    (skip_part,) = call(
        functools.partial(skip_back_of, width),
        [shape((row_count, units), F32)],
        skip_weight,
        *grads,
        flops=2 * row_count * units * out_width,
    )
    input_total = (kept_t[0, 0] + arrived_t[0, 0].astype(F32)).T + skip_part

    outbias_part = jnp.concatenate(
        [
            jnp.sum(grads[2 * c], axis=0, dtype=F32) + jnp.sum(grads[2 * c + 1], axis=0, dtype=F32)
            for c in range(chunks)
        ]
    )
    bias_block = halve_small(
        jnp.concatenate(
            [inbias_part[:, 0].reshape(data_size, -1), outbias_part.reshape(data_size, -1)], 1
        ),
        "dp",
    )
    rescale = 1.0 / (window_count * data_size)
    inner_total, outer_total, skip_total = call(
        functools.partial(last_sums, rescale),
        [shape((share, depth), F32)] + [shape((share, out_width), F32)] * 2,
        *[k for k, _ in halved],
        *[a for _, a in halved],
        flops=3 * share * depth,
    )
    return (
        input_total,
        inner_total,
        outer_total,
        skip_total,
        bias_block[:share] * rescale,
        bias_block[share:] * rescale,
    )


def skip_back_of(width, weight, *refs):
    skip_back(weight, width, *refs)


def solution(mesh):
    in_specs = (
        P("dp", None),
        P("mp", None),
        P("mp"),
        P("mp", None),
        P("mp", None),
        P(),
        P("dp", None),
        P(),
        P("dp"),
    )
    out_specs = (
        P("dp", "mp"),
        P(("mp", "dp"), None),
        P(("mp", "dp"), None),
        P(("mp", "dp"), None),
        P(("mp", "dp")),
        P("dp"),
    )
    return jax.shard_map(
        on_device, mesh=mesh, in_specs=in_specs, out_specs=out_specs, check_vma=False
    )
```

```python
import functools

import jax
import jax.numpy as jnp
from jax import lax
from jax.experimental import pallas as pl
from jax.experimental.pallas import tpu as pltpu
from jax.sharding import PartitionSpec as P

LEVELS = 9


huber_width = 0.5


F32, BF16, F16 = jnp.float32, jnp.bfloat16, jnp.float16
LANES = 128
TAIL = 8
WIRE_SCALE = 0.25
ON_LAST = (((1,), (1,)), ((), ()))
IN_VMEM = pl.BlockSpec(memory_space=pltpu.VMEM)
ANYWHERE = pl.BlockSpec(memory_space=pl.ANY)
IN_HBM = pl.BlockSpec(memory_space=pltpu.HBM)


def dot(a, b):
    return jnp.dot(a, b, preferred_element_type=F32)


def dot_last(a, b):
    return lax.dot_general(a, b, ON_LAST, preferred_element_type=F32)


def round_up(value, step):
    return -(-value // step) * step


def shape(dims, dtype):
    return jax.ShapeDtypeStruct(dims, dtype)


def call(body, shapes, *args, flops, after=(), scratch=(), vmem=12 << 20, specs=None):
    inputs, extra = len(args), len(after)

    def run(*refs):
        body(*refs[:inputs], *refs[inputs + extra :])

    moved = sum(a.size * a.dtype.itemsize for a in args)
    moved += sum(s.size * s.dtype.itemsize for s in shapes)
    return pl.pallas_call(
        run,
        out_shape=tuple(shapes),
        in_specs=list(specs or [IN_VMEM] * inputs) + [ANYWHERE] * extra,
        out_specs=tuple(IN_VMEM for _ in shapes),
        scratch_shapes=list(scratch),
        cost_estimate=pl.CostEstimate(
            flops=int(flops), bytes_accessed=int(moved), transcendentals=0
        ),
        compiler_params=pltpu.CompilerParams(vmem_limit_bytes=vmem),
    )(*args, *after)


def swap(value, axis, distance):
    size = lax.axis_size(axis)
    return lax.ppermute(value, axis, [(i, i ^ distance) for i in range(size)])


class Window:
    def __init__(self, width, parts):
        self.gaps = sorted({(part * width) % LANES for part in range(parts)})
        self.at = round_up(width, LANES)
        self.width = round_up(width + self.gaps[-1], LANES)
        self.total = self.at + self.width

    def place(self, part, width):
        first = part * width
        start = first // LANES * LANES
        return pl.multiple_of(start, LANES), first - start


def core_rows(half, own):
    core = lax.axis_index("mp") % 2
    which = core if own else 1 - core
    return pl.multiple_of(which * half, half)


def forward(
    window, width, series, wi, bias, wo, ws, joined, slope_in, joined_w, sent, kept,
    series_v, wi_v, sems,
):
    units = wi.shape[0]
    part = lax.axis_index("mp")
    half = series.shape[0] // 2
    start, gap = window.place(part, units)
    starts = [core_rows(half, False), core_rows(half, True)]
    copies = [
        pltpu.make_async_copy(series.at[pl.ds(starts[0], half), :], series_v.at[0], sems.at[0]),
        pltpu.make_async_copy(wi, wi_v, sems.at[1]),
        pltpu.make_async_copy(wo, joined_w.at[pl.ds(0, units), :], sems.at[2]),
        pltpu.make_async_copy(
            ws,
            joined_w.at[pl.ds(pl.multiple_of(window.at + gap, 16), units), :],
            sems.at[3],
        ),
        pltpu.make_async_copy(series.at[pl.ds(starts[1], half), :], series_v.at[1], sems.at[4]),
    ]
    for copy in copies:
        copy.start()

    def clear(first, last):
        if last > first:
            joined_w[first:last, :] = jnp.zeros((last - first, joined_w.shape[1]), BF16)

    clear(units, window.at)
    for g in window.gaps:

        @pl.when(gap == g)
        def _():
            clear(window.at, window.at + g)
            clear(window.at + g + units, window.total)

    for side, target in ((0, sent), (1, kept)):
        rows = pl.ds(starts[side], half)
        if side == 0:
            copies[0].wait()
            copies[1].wait()
        else:
            copies[4].wait()
        preact = dot_last(series_v[side], wi_v[...]) + bias[...]
        sigmoids = 1.0 / (1.0 + jnp.exp(-preact))
        slope_in[rows, :] = sigmoids * (1.0 + preact * (1.0 - sigmoids))
        if units < window.at:
            joined[rows, units : window.at] = jnp.zeros((half, window.at - units), BF16)
        joined[rows, 0:units] = (preact * sigmoids).astype(BF16)
        joined[rows, window.at : window.total] = series_v[side, :, pl.ds(start, window.width)]
        if side == 0:
            copies[2].wait()
            copies[3].wait()
        target[...] = dot(joined[rows, :], joined_w[:, 0:width])


def forward_more(first, joined, joined_w, sent, kept):
    half = sent.shape[0]
    for own, target in ((False, sent), (True, kept)):
        rows = pl.ds(core_rows(half, own), half)
        target[...] = dot(joined[rows, :], joined_w[:, first : first + target.shape[1]])


def prepare(patch_count, targets, level, counts, *outs):
    tau, outs = outs[0], outs[1:]
    half = outs[0].shape[0]
    horizon = targets.shape[1]
    quantiles = level.shape[1]
    base = core_rows(half, True)
    channel = lax.rem(lax.broadcasted_iota(jnp.int32, tau.shape, 1), quantiles)
    picked = jnp.zeros(tau.shape, jnp.int32)
    for c in range(quantiles):
        picked = jnp.where(channel == c, level[0:1, c : c + 1], picked)
    tau[...] = (picked.astype(F32) + 1.0) / (LEVELS + 1)
    count = counts[...]
    inverse = 1.0 / count.astype(F32)
    row = lax.broadcasted_iota(jnp.int32, (half, count.shape[1]), 0) + base
    opens = lax.broadcasted_iota(jnp.int32, (half, count.shape[1]), 1) * patch_count
    inside = (row >= opens) & (row < opens + count)
    weights = jnp.sum(jnp.where(inside, inverse, 0.0), axis=1, keepdims=True)
    target = targets[pl.ds(base, half), :]
    high = target.astype(BF16)
    rest = target - high.astype(F32)
    middle = rest.astype(BF16)
    low = (rest - middle.astype(F32)).astype(BF16)
    first_col = 0
    for spread, weight in zip(outs[0::2], outs[1::2]):
        width = spread.shape[1]
        columns = lax.broadcasted_iota(jnp.int32, (horizon, width), 1) + first_col
        lowest = lax.broadcasted_iota(jnp.int32, (horizon, width), 0) * quantiles
        chosen = jnp.where((columns >= lowest) & (columns < lowest + quantiles), 1.0, 0.0)
        chosen = chosen.astype(BF16)
        spread[...] = dot(high, chosen) + dot(middle, chosen) + dot(low, chosen)
        weight[...] = jnp.broadcast_to(weights, weight.shape)
        first_col += width


def output_slope(own, other, bias, spread, tau, weights):
    summed = (own.astype(F32) + other.astype(F32)) * (1.0 / WIRE_SCALE)
    residue = spread - (summed + bias)
    slopes = jnp.where(residue >= 0, tau, 1.0 - tau) * jnp.clip(
        residue / huber_width, -1.0, 1.0
    )
    return (-slopes * weights).astype(BF16)


def on_bit(axis, distance, body):
    bit = (lax.axis_index(axis) // distance) % 2
    for value in range(2):

        @pl.when(bit == value)
        def _():
            body(value)


def outer_sums(window, units, joined_t, mine, theirs, sent, kept, sums, total):
    half = mine.shape[0]
    share = kept.shape[2]
    _, gap = window.place(lax.axis_index("mp"), units)
    own = pl.ds(core_rows(half, True), half)
    far = pl.ds(core_rows(half, False), half)
    for at, first in ((0, 0), (1, pl.multiple_of(window.at + gap, 16))):
        rows = pl.ds(first, units)
        total[at] = dot(joined_t[rows, own], mine[...]) + dot(joined_t[rows, far], theirs[...])

    def deal(bit):
        for at in range(2):
            for pair in range(kept.shape[1]):
                for target, which in ((sent, 1 - bit), (kept, bit)):
                    at_row = (2 * pair + which) * share
                    target[at, pair] = total[at, at_row : at_row + share, :].astype(target.dtype)

    on_bit("dp", 1, deal)
    ones = jnp.ones((TAIL, half), BF16)
    sums[...] = dot(ones, mine[...]) + dot(ones, theirs[...])


def back(first, weight, mine, theirs, flow):
    half, width = mine.shape
    for grads, own in ((mine, True), (theirs, False)):
        cols = pl.ds(core_rows(half, own), half)
        flow[:, cols] = dot_last(weight[:, first : first + width], grads[...])


def back_more(first, weight, mine, theirs, before, flow):
    half, width = mine.shape
    for grads, own in ((mine, True), (theirs, False)):
        cols = pl.ds(core_rows(half, own), half)
        flow[:, cols] = before[:, cols] + dot_last(
            weight[:, first : first + width], grads[...]
        )


def put_tail(tail, sent, kept, first):
    kept[first : first + TAIL, :] = tail
    high = tail.astype(BF16).astype(F32)
    row = lax.broadcasted_iota(jnp.int32, tail.shape, 0)
    low = pltpu.roll(tail - high, 2, 0)
    mixed = jnp.where(row < 2, high, jnp.where(row < 4, low, 0.0))
    sent[first : first + TAIL, :] = mixed.astype(BF16)


def join_tail(kept, arrived, first):
    tail = arrived[first : first + TAIL, :].astype(F32)
    return kept[first : first + TAIL, :] + (tail + pltpu.roll(tail, TAIL - 2, 0))


def hidden_back(first, sums_count, weight, mine, theirs, flow, slope_t, series, *rest):
    sums, (grad_t, sent, kept, total, tail) = rest[:sums_count], rest[sums_count:]
    half, width = mine.shape
    units = grad_t.shape[0]
    for grads, own in ((mine, True), (theirs, False)):
        cols = pl.ds(core_rows(half, own), half)
        flown = flow[:, cols] + dot_last(weight[:, first : first + width], grads[...])
        grad_t[:, cols] = (flown * slope_t[:, cols]).astype(BF16)
    total[...] = dot(grad_t[...], series[...])
    blocks = kept.shape[0] - TAIL
    share = units // lax.axis_size("dp")

    def deal(bit):
        for pair in range(blocks // share):
            for target, which in ((sent, 1 - bit), (kept, bit)):
                at_row = (2 * pair + which) * share
                target[pair * share : (pair + 1) * share, :] = total[
                    at_row : at_row + share, :
                ].astype(target.dtype)

    on_bit("dp", 1, deal)
    tail[...] = jnp.zeros_like(tail)
    at = 0
    for part in sums:
        tail[0:1, at : at + part.shape[1]] = part[0:1, :]
        at += part.shape[1]
    ones = jnp.ones((TAIL, grad_t.shape[1]), BF16)
    tail[1:2, 0:units] = dot_last(ones, grad_t[...])[0:1, :]
    put_tail(tail[...], sent, kept, blocks)


def inner_step(share, distance, blocks, arrived, sent, kept):
    count = kept.shape[0] - TAIL

    def deal(bit):
        for pair in range(count // share):
            for target, which in ((sent, 1 - bit), (kept, bit)):
                at_row = (2 * pair + which) * share
                rows = slice(at_row, at_row + share)
                target[pair * share : (pair + 1) * share, :] = (
                    blocks[rows, :] + arrived[rows, :].astype(F32)
                ).astype(target.dtype)

    on_bit("dp", distance, deal)
    put_tail(join_tail(blocks, arrived, blocks.shape[0] - TAIL), sent, kept, count)


def halve_step(axis, distance, blocks, arrived, sent, kept):
    bit = (lax.axis_index(axis) // distance) % 2
    for at in range(kept.shape[0]):
        for pair in range(kept.shape[1]):
            for target, which in ((sent, 1 - bit), (kept, bit)):
                index = 2 * pair + which
                target[at, pair] = (
                    blocks[at, index] + arrived[at, index].astype(F32)
                ).astype(target.dtype)


def input_parts(weight_t, grad_t, sent, kept):
    core = lax.axis_index("mp") % 2
    width = kept.shape[2]
    for pair in range(kept.shape[1]):
        for target, which in ((sent, 1 - core), (kept, core)):
            rows = pl.ds(pl.multiple_of((2 * pair + which) * width, 16), width)
            target[0, pair] = dot(weight_t[rows, :], grad_t[...]).astype(target.dtype)


def input_last(kept, arrived, skip, out):
    out[...] = kept[0, 0] + arrived[0, 0].astype(F32) + skip[...]


def last_sums(rescale, *refs):
    count = (len(refs) - 4) // 2
    kept, arrived, outs = refs[:count], refs[count : 2 * count], refs[2 * count :]
    share = outs[0].shape[0]
    outs[0][...] = (kept[0][0:share, :] + arrived[0][0:share, :].astype(F32)) * rescale
    outs[3][...] = join_tail(kept[0], arrived[0], share) * rescale
    for at in range(2):
        first = 0
        for k, a in zip(kept[1:], arrived[1:]):
            cols = slice(first, first + k.shape[3])
            outs[1 + at][:, cols] = (k[at, 0] + a[at, 0].astype(F32)) * rescale
            first += k.shape[3]


class Halving:
    def __init__(self, sent, kept, axis, share=None):
        self.axis, self.share, self.distance = axis, share, 1
        self.kept = kept
        self.arrived = swap(sent, axis, 1)

    def done(self):
        return 2 * self.distance >= lax.axis_size(self.axis)

    def step(self, after):
        self.distance *= 2
        if self.share is None:
            dims = (self.kept.shape[0], self.kept.shape[1] // 2) + self.kept.shape[2:]
            body = functools.partial(halve_step, self.axis, self.distance)
        else:
            dims = ((self.kept.shape[0] - TAIL) // 2 + TAIL, self.kept.shape[1])
            body = functools.partial(inner_step, self.share, self.distance)
        sent, kept = call(
            body,
            (shape(dims, BF16), shape(dims, F32)),
            self.kept,
            self.arrived,
            flops=self.kept.size,
            after=after,
        )
        self.kept, self.arrived = kept, swap(sent, self.axis, self.distance)
        return sent


def chunk_widths(width):
    tiles = width // LANES
    first = tiles // 2
    return [first * LANES, width - first * LANES]


def on_device(
    series, inner_weight, inner_bias, outer_weight, skip_weight, outer_bias, targets, levels, counts
):
    row_count, depth = series.shape
    window_count = counts.shape[0]
    patch_count = row_count // window_count
    out_width = outer_weight.shape[1]
    units = inner_weight.shape[0]
    model_size = lax.axis_size("mp")
    data_size = lax.axis_size("dp")
    half = row_count // 2
    window = Window(units, model_size)
    widths = chunk_widths(out_width)
    firsts = [sum(widths[:c]) for c in range(len(widths))]
    pairs = data_size // 2
    share = units // data_size

    joined, slope_in, joined_w, sent, kept = call(
        functools.partial(forward, window, widths[0]),
        [
            shape((row_count, window.total), BF16),
            shape((row_count, units), F32),
            shape((window.total, out_width), BF16),
            shape((half, widths[0]), F32),
            shape((half, widths[0]), F32),
        ],
        series,
        inner_weight,
        inner_bias.reshape(1, units),
        outer_weight,
        skip_weight,
        flops=2 * row_count * depth * units + 2 * row_count * window.total * widths[0],
        vmem=24 << 20,
        specs=[IN_HBM, IN_HBM, IN_VMEM, IN_HBM, IN_HBM],
        scratch=[
            pltpu.VMEM((2, half, depth), BF16),
            pltpu.VMEM((units, depth), BF16),
            pltpu.SemaphoreType.DMA((5,)),
        ],
    )
    shares = [(sent, kept)]
    for first, width in zip(firsts[1:], widths[1:]):
        shares.append(
            call(
                functools.partial(forward_more, first),
                [shape((half, width), F32)] * 2,
                joined,
                joined_w,
                flops=2 * row_count * window.total * width,
            )
        )
    own = [((kept + swap(sent, "mp", 1)) * WIRE_SCALE).astype(F16) for sent, kept in shares]
    other = [swap(value, "mp", 2) for value in own]
    joined_t = joined.T
    slope_t = slope_in.T
    inner_t = inner_weight.T
    spread_shapes = [shape((half, w), F32) for w in widths for _ in range(2)]
    tau, *spreads = call(
        functools.partial(prepare, patch_count),
        [shape((1, out_width), F32), *spread_shapes],
        targets,
        levels.reshape(1, -1),
        counts.reshape(1, -1),
        flops=6 * half * targets.shape[1] * out_width,
        after=(joined_t, slope_t, inner_t),
    )

    grads, outers, sums = [], [], []
    flow = skip_t = None
    order = ()
    for chunk, (first, width) in enumerate(zip(firsts, widths)):
        cols = slice(first, first + width)
        mine = output_slope(
            own[chunk],
            other[chunk],
            outer_bias[cols],
            spreads[2 * chunk],
            tau[:, cols],
            spreads[2 * chunk + 1],
        )
        theirs = swap(mine, "mp", 1)
        dims = (2, pairs, share, width)
        sent, kept, summed = call(
            functools.partial(outer_sums, window, units),
            [shape(dims, BF16), shape(dims, F32), shape((TAIL, width), F32)],
            joined_t,
            mine,
            theirs,
            flops=4 * row_count * units * width,
            scratch=[pltpu.VMEM((2, units, width), F32)],
            after=order,
        )
        sums.append(summed)
        outers.append(Halving(sent, kept, "dp"))
        if chunk < len(widths) - 1:
            body = back if flow is None else back_more
            (flow,) = call(
                functools.partial(body, first),
                [shape((units, row_count), F32)],
                outer_weight,
                mine,
                theirs,
                *([] if flow is None else [flow]),
                flops=2 * row_count * units * width,
                after=(sent,),
            )
            body = back if skip_t is None else back_more
            (skip_t,) = call(
                functools.partial(body, first),
                [shape((units, row_count), F32)],
                skip_weight,
                mine,
                theirs,
                *([] if skip_t is None else [skip_t]),
                flops=2 * row_count * units * width,
                after=(flow,),
            )
            order = (skip_t,)
    dims = (pairs * share + TAIL, depth)
    grad_t, sent, kept = call(
        functools.partial(hidden_back, firsts[-1], len(sums)),
        [shape((units, row_count), BF16), shape(dims, BF16), shape(dims, F32)],
        outer_weight,
        mine,
        theirs,
        flow,
        slope_t,
        series,
        *sums,
        flops=2 * row_count * units * (widths[-1] + depth),
        scratch=[pltpu.VMEM((units, depth), F32), pltpu.VMEM((TAIL, depth), F32)],
        after=(sent,),
    )
    inner = Halving(sent, kept, "dp", share)
    dims = (1, model_size // 2, units, row_count)
    sent, kept = call(
        input_parts,
        [shape(dims, BF16), shape(dims, F32)],
        inner_t,
        grad_t,
        flops=2 * row_count * units * depth,
        after=(sent,),
    )
    inputs = Halving(sent, kept, "mp")
    order = sent
    order = outers[0].step((order,))
    order = inputs.step((order,))
    (skip_t,) = call(
        functools.partial(back_more, firsts[-1]),
        [shape((units, row_count), F32)],
        skip_weight,
        mine,
        theirs,
        skip_t,
        flops=2 * row_count * units * widths[-1],
        after=(order,),
    )
    order = skip_t
    queue = outers + [inner]
    while not all(item.done() for item in queue):
        for item in sorted(queue, key=lambda i: (i.distance, queue.index(i))):
            if not item.done():
                order = item.step((order,))
                break
    (input_t,) = call(
        input_last,
        [shape((units, row_count), F32)],
        inputs.kept,
        inputs.arrived,
        skip_t,
        flops=2 * row_count * units,
        after=(order,),
    )
    rescale = 1.0 / (window_count * data_size)
    halved = [inner, *outers]
    inner_total, outer_total, skip_total, bias_total = call(
        functools.partial(last_sums, rescale),
        [shape((share, depth), F32)]
        + [shape((share, out_width), F32)] * 2
        + [shape((TAIL, depth), F32)],
        *[item.kept for item in halved],
        *[item.arrived for item in halved],
        flops=3 * share * depth,
        after=(input_t,),
    )
    data_index = lax.axis_index("dp")
    bias_share = out_width // data_size
    return (
        input_t.T,
        inner_total,
        outer_total,
        skip_total,
        lax.dynamic_slice_in_dim(bias_total[1], data_index * share, share),
        lax.dynamic_slice_in_dim(bias_total[0], data_index * bias_share, bias_share),
    )


def solution(mesh):
    in_specs = (
        P("dp", None),
        P("mp", None),
        P("mp"),
        P("mp", None),
        P("mp", None),
        P(),
        P("dp", None),
        P(),
        P("dp"),
    )
    out_specs = (
        P("dp", "mp"),
        P(("mp", "dp"), None),
        P(("mp", "dp"), None),
        P(("mp", "dp"), None),
        P(("mp", "dp")),
        P("dp"),
    )
    return jax.shard_map(
        on_device, mesh=mesh, in_specs=in_specs, out_specs=out_specs, check_vma=False
    )
```
